32 devices in a mesh: groups: 2 (over y), tp: 4 (over z), tq: 2 (over x), tr: 2 (over core).
Axes of the slice: x: 2, y: 2, z: 4, core: 2. Of those that a mesh axis runs over, the one named last changes fastest.
Arguments:
- attn_heads: bfloat16 [128, 16384], P('groups', ('tp', 'tq', 'tr')), parts along dimension 0, may hold values from -6 to 6
- residual: bfloat16 [128, 16384], P('groups', ('tp', 'tq', 'tr')), parts along dimension 0, may hold values from -120 to 120
- o_weight: bfloat16 [16384, 16384], P(('tp', 'tq', 'tr')), may hold values from -0.0625 to 0.0625
- norm_gain: bfloat16 [16384], P(('tp', 'tq', 'tr')), may hold values from 0.099609375 to 1.8984375
- q_weight: bfloat16 [16384, 16384], P(None, ('tp', 'tq', 'tr')), may hold values from -0.046875 to 0.046875
Outputs:
- hidden: bfloat16 [128, 16384], P('groups', ('tp', 'tq', 'tr')), parts along dimension 0
- peak_value: float32 [128], P('groups'), parts along dimension 0
- query: bfloat16 [128, 16384], P('groups', ('tp', 'tq', 'tr')), parts along dimension 0
The draws below stay inside these ranges and needn't reach their ends.
There are 2 independent parts, one for each index of `groups`. The reference program is written for one: setup_inputs(seed, part) draws one part's arguments, and reference() takes and returns one part's arrays. A program takes and returns all parts, laid end to end along the dimension named above; an argument that names none is the same for every part. Nothing has to cross between parts.
All inputs are finite; a program needn't handle non-finite values. Where the reference program divides by a largest or mean magnitude, that divisor is 1e-20 or more.
Results may differ from the reference program's by a relative error of at most 0.0095.
Values may be sent and summed in bfloat16 or wider, within the bound.
A program may use at most 128 MiB of HBM per device.

```python
import jax
import jax.numpy as jnp
from jax import lax

D = 16384
TOK = 64
QD = 16384


def draw_residual(key, part):
    keys = jax.random.split(jax.random.fold_in(key, 11), 3)
    row_scale = jnp.exp(jax.random.uniform(keys[0], (TOK, 1), jnp.float32) * jnp.log(10.0))
    col_random = jnp.exp(jax.random.uniform(keys[1], (1, D), jnp.float32, jnp.log(0.5), jnp.log(5.0)))
    col_rise = jnp.exp(jnp.arange(D, dtype=jnp.float32)[None, :] / D * jnp.log(3.0))
    base_values = jax.random.normal(keys[2], (TOK, D), jnp.float32)
    base_values = jnp.clip(base_values, -4.0, 4.0)
    return (0.2 * base_values * row_scale * col_random * col_rise).astype(jnp.bfloat16)


def with_spikes(result, rng, source, target, blocks, factor):
    def block_of(axis_at):
        return (jnp.arange(result.shape[axis_at]) // (result.shape[axis_at] // blocks)).reshape((-1,) + (1,) * (result.ndim - 1 - axis_at))

    first = jax.random.permutation(rng, blocks)[block_of(target)]
    second = (block_of(target) + blocks // 2) % blocks
    return jnp.where((block_of(source) == first) | (block_of(source) == second), factor * result, result)


def shard_levels(key, shape, pieces, smallest, largest):
    level, own = 1.0, jax.random.fold_in(key, 6)
    for dim, blocks in pieces:
        steps = jnp.exp(jax.random.uniform(jax.random.fold_in(own, dim), (blocks,), jnp.float32, smallest / len(pieces), largest / len(pieces)))
        level = level * jnp.repeat(steps, shape[dim] // blocks).reshape([-1 if axis == dim else 1 for axis in range(len(shape))])
    return level


def normal_values(own_key, extent, spread, limit, shards=(), held_as=jnp.bfloat16):
    drawn = spread * jax.random.normal(own_key, extent, jnp.float32)
    if shards:
        drawn = drawn * shard_levels(own_key, extent, shards, -0.22, 0.18)
    return jnp.clip(drawn, -limit, limit).astype(held_as)


def heavy_noise(rng, extent, scale, most, shards, heavy, kind=jnp.bfloat16):
    result = scale * jax.random.normal(rng, extent, jnp.float32)
    if shards:
        result = result * shard_levels(rng, extent, shards, -0.22, 0.18)
    return jnp.clip(with_spikes(result, jax.random.fold_in(rng, 3), *heavy), -most, most).astype(kind)


def setup_inputs(seed: int = 0, part: int = 0) -> dict:
    seeds = jax.random.split(jax.random.key(seed), 6)
    part_keys = jax.random.split(jax.random.fold_in(seeds[5], part), 6)
    return {
        "attn_heads": normal_values(part_keys[0], (TOK, QD), 1.0, 6.0, ((1, 16),)),
        "residual": draw_residual(jax.random.fold_in(jax.random.fold_in(seeds[5], part), 71), part),
        "o_weight": heavy_noise(seeds[2], (QD, D), QD ** -0.5, 0.0625, ((0, 16),), (0, 1, 16, 2.0)),
        "norm_gain": jnp.clip(1.0 + 0.18 * jax.random.normal(seeds[3], (D,), jnp.float32), 0.099609375, 1.8984375).astype(jnp.bfloat16),
        "q_weight": normal_values(seeds[4], (D, QD), D ** -0.5, 0.046875, ((1, 16),)),
    }


def reference(attn_heads, residual, o_weight, norm_gain, q_weight):
    attn_total = jnp.dot(attn_heads, o_weight, preferred_element_type=jnp.float32)
    hidden = (residual.astype(jnp.float32) + attn_total).astype(jnp.bfloat16)
    widened = hidden.astype(jnp.float32)
    inv_rms = lax.rsqrt(lax.optimization_barrier(jnp.sum(widened * widened, axis=1)) / D + 1e-05)
    normed = widened * norm_gain.astype(jnp.float32) * inv_rms[:, None]
    peak_value = lax.optimization_barrier(jnp.max(jnp.abs(normed), axis=1))
    quantized = (normed * (448.0 / (peak_value + 1e-06))[:, None]).astype(jnp.bfloat16)
    projected = jnp.dot(quantized, q_weight, preferred_element_type=jnp.float32)
    query = (projected * ((peak_value + 1e-06) / 448.0)[:, None]).astype(jnp.bfloat16)
    return (hidden, peak_value, query)
```

```python
import functools

import jax
import jax.numpy as jnp
from jax import lax
from jax.experimental import pallas as pl
from jax.experimental.pallas import tpu as pltpu
from jax.sharding import PartitionSpec as P

MESH = pl.DeviceIdType.MESH
F32, BF16 = jnp.float32, jnp.bfloat16
SLOTS = 8
LAG = 4


def flip(index, mask):
    bit = 1
    while bit <= mask:
        if mask & bit:
            index = index + bit - 2 * bit * ((index // bit) % 2)
        bit *= 2
    return index


def multiply(lhs_ref, rhs_ref, put):
    width = rhs_ref.shape[1]
    tile = min(width, 512)

    def step(j, carry):
        columns = pl.ds(pl.multiple_of(j * tile, tile), tile)
        put(columns, jnp.dot(lhs_ref[...], rhs_ref[:, columns], preferred_element_type=F32))
        return carry

    lax.fori_loop(0, width // tile, step, 0)


def kernel(
    Z, X, C, D,
    attn_hbm, res_hbm, o_hbm, gain_ref, q_hbm,
    hidden_hbm, peak_ref, query_ref,
    attn, res, hid, obuf, qbuf, gath, acc, total,
    core_out, core_in, x_out, x_in, z_out, z_in, stat_out, stat_in,
    small_sem, o_sem, q_sem, core_s, core_r, x_s, x_r, z_s, z_r, g_s, g_r, st_s, st_r,
):
    TOK, F = res.shape
    n = Z * X * C
    me = {"tp": lax.axis_index("tp"), "tq": lax.axis_index("tq"), "tr": lax.axis_index("tr")}

    def block_of(dz, dx, dc):
        return (flip(me["tp"], dz) * X + flip(me["tq"], dx)) * C + flip(me["tr"], dc)

    def send(src, dst, s, r, axis, d):
        copy = pltpu.make_async_remote_copy(
            src_ref=src, dst_ref=dst, send_sem=s, recv_sem=r,
            device_id={axis: flip(me[axis], d)}, device_id_type=MESH,
        )
        copy.start()
        sent.append(copy)
        return copy

    sent = []
    groups = [(dz, dx) for dz in reversed(range(Z)) for dx in reversed(range(X))]
    order = [(dz, dx, dc) for dz, dx in groups for dc in reversed(range(C))]

    def o_copy(b):
        start = pl.multiple_of(block_of(*order[b]) * F, F)
        return pltpu.make_async_copy(
            o_hbm.at[:, pl.ds(start, F)], obuf.at[b % SLOTS], o_sem.at[b % SLOTS])

    def slot(dz, dx, dc):
        return (dz * X + dx) * C + dc

    def blocks_from_z(dz):
        later = [(dz, dx, 0) for dx in range(1, X)]
        return later + [(dz, dx, dc) for dx in range(X) for dc in range(1, C)]

    use = [(0, 0, 0)]
    for dz in range(1, Z):
        use += [(dz, 0, 0)] + blocks_from_z(dz - 1)
    use += blocks_from_z(Z - 1)

    def q_copy(k):
        start = pl.multiple_of(block_of(*use[k]) * F, F)
        at = slot(*use[k])
        return pltpu.make_async_copy(q_hbm.at[pl.ds(start, F), :], qbuf.at[at], q_sem.at[at])

    attn_copy = pltpu.make_async_copy(attn_hbm, attn, small_sem.at[0])
    attn_copy.start()
    for b in range(min(SLOTS, n)):
        o_copy(b).start()
    res_copy = pltpu.make_async_copy(res_hbm, res, small_sem.at[1])
    res_copy.start()

    barrier = pltpu.get_barrier_semaphore()
    for axis, size in (("tp", Z), ("tq", X), ("tr", C)):
        for d in range(1, size):
            pl.semaphore_signal(
                barrier, inc=1, device_id={axis: flip(me[axis], d)}, device_id_type=MESH)
    attn_copy.wait()

    core_copies, x_copies, z_copies = {}, {}, {}
    q_next = 0

    def after_core(i):
        dz, dx = groups[i]
        value = acc[i]
        for dc in range(1, C):
            core_copies[i, dc].wait_recv()
            value = value + core_in[i * (C - 1) + dc - 1].astype(F32)
        if dx:
            at = dz * (X - 1) + dx - 1
            x_out[at] = value.astype(BF16)
            x_copies[dz, dx] = send(x_out.at[at], x_in.at[at], x_s.at[at], x_r.at[at], "tq", dx)
        else:
            acc[i] = value

    def after_x(dz):
        i = groups.index((dz, 0))
        value = acc[i]
        for dx in range(1, X):
            x_copies[dz, dx].wait_recv()
            value = value + x_in[dz * (X - 1) + dx - 1].astype(F32)
        if dz:
            z_out[dz - 1] = value.astype(BF16)
            z_copies[dz] = send(
                z_out.at[dz - 1], z_in.at[dz - 1], z_s.at[dz - 1], z_r.at[dz - 1], "tp", dz)
        else:
            total[...] = value

    pending = []
    for i, (dz, dx) in enumerate(groups):
        for dc in reversed(range(C)):
            b = i * C + C - 1 - dc
            o_copy(b).wait()
            rhs = obuf.at[b % SLOTS]
            if dc:
                at = i * (C - 1) + dc - 1

                def put(columns, product):
                    core_out[at, :, columns] = product.astype(BF16)

                multiply(attn, rhs, put)
                if b == 0:
                    pl.semaphore_wait(barrier, Z + X + C - 3)
                core_copies[i, dc] = send(
                    core_out.at[at], core_in.at[at], core_s.at[at], core_r.at[at], "tr", dc)
            else:

                def put(columns, product):
                    acc[i, :, columns] = product

                multiply(attn, rhs, put)
            if b + SLOTS < n:
                o_copy(b + SLOTS).start()
            else:
                q_copy(q_next).start()
                q_next += 1
        if i >= 1:
            after_core(i - 1)
            if groups[i - 1][1] == 0:
                pending.append((i - 1, groups[i - 1][0]))
        if pending and i - pending[0][0] >= LAG:
            after_x(pending.pop(0)[1])
    while q_next < n:
        q_copy(q_next).start()
        q_next += 1
    after_core(len(groups) - 1)
    pending.append((len(groups) - 1, 0))
    for _, dz in pending:
        after_x(dz)

    res_copy.wait()
    value = total[...]
    for dz in range(1, Z):
        z_copies[dz].wait_recv()
        value = value + z_in[dz - 1].astype(F32)
    hidden = (res[...].astype(F32) + value).astype(BF16)
    hid[...] = hidden
    widened = hidden.astype(F32)
    gained = widened * gain_ref[...].astype(F32)
    gath[0] = gained.astype(BF16)

    arrive = {}

    def forward(dz, dx):
        at = slot(dz, dx, 0)
        for dc in range(1, C):
            to = slot(dz, dx, dc)
            arrive[dz, dx, dc] = send(
                gath.at[at], gath.at[to], g_s.at[to], g_r.at[to], "tr", dc)

    def forward_x(dz):
        at = slot(dz, 0, 0)
        for dx in range(1, X):
            to = slot(dz, dx, 0)
            arrive[dz, dx, 0] = send(
                gath.at[at], gath.at[to], g_s.at[to], g_r.at[to], "tq", dx)

    for dz in range(1, Z):
        to = slot(dz, 0, 0)
        arrive[dz, 0, 0] = send(gath.at[0], gath.at[to], g_s.at[to], g_r.at[to], "tp", dz)
    forward_x(0)
    forward(0, 0)
    hidden_copy = pltpu.make_async_copy(hid, hidden_hbm, small_sem.at[2])
    hidden_copy.start()

    squares = jnp.sum(widened * widened, axis=1, keepdims=True)
    top = jnp.max(jnp.abs(gained), axis=1, keepdims=True)
    wide = jnp.concatenate(
        [jnp.broadcast_to(squares, (TOK, 128)), jnp.broadcast_to(top, (TOK, 128))], axis=0)
    stat = jnp.transpose(wide)[:8, :]
    lane = lax.broadcasted_iota(jnp.int32, stat.shape, 1)
    axes = (("tr", C), ("tq", X), ("tp", Z))
    first = {"tr": 0, "tq": C - 1, "tp": C + X - 2}
    stat_copies = {}

    def stat_send(stage, stat):
        axis, size = axes[stage]
        stat_out[stage] = stat
        for d in range(1, size):
            at = first[axis] + d - 1
            stat_copies[axis, d] = send(
                stat_out.at[stage], stat_in.at[at], st_s.at[at], st_r.at[at], axis, d)

    def stat_take(stage, stat):
        axis, size = axes[stage]
        for d in range(1, size):
            stat_copies[axis, d].wait_recv()
            other = stat_in[first[axis] + d - 1]
            stat = jnp.where(lane < TOK, stat + other, jnp.maximum(stat, other))
        return stat

    stat_send(0, stat)

    for k, at in enumerate(use):
        dz, dx, dc = at
        if k:
            arrive[at].wait_recv()
            if dc == 0:
                if dx == 0:
                    forward_x(dz)
                forward(dz, dx)
        q_copy(k).wait()
        if k == 0:

            def put(columns, product):
                total[:, columns] = product
        else:

            def put(columns, product):
                total[:, columns] += product

        multiply(gath.at[slot(*at)], qbuf.at[slot(*at)], put)
        if k in (1, 3):
            stage = 0 if k == 1 else 1
            stat = stat_take(stage, stat_out[stage])
            stat_send(stage + 1, stat)
    stat = stat_take(2, stat_out[2])
    scale = lax.rsqrt(stat / D + 1e-05)
    peak_ref[...] = pltpu.roll(stat, TOK, 1) * scale
    rows = jnp.transpose(jnp.broadcast_to(scale[:1, :], (128, 128)))[:TOK, :1]
    query_ref[...] = (total[...] * rows).astype(BF16)
    hidden_copy.wait()
    for copy in sent:
        copy.wait_send()


def body(sizes, attn_heads, residual, o_weight, norm_gain, q_weight):
    Z, X, C = sizes
    TOK, F = residual.shape
    K, D = o_weight.shape
    n = Z * X * C
    pairs = Z * X * (C - 1)
    dma = pltpu.SemaphoreType.DMA
    block = (TOK, F)
    hbm = pl.BlockSpec(memory_space=pl.ANY)
    vmem = pl.BlockSpec(memory_space=pltpu.VMEM)
    hops = C + X + Z - 3
    hidden, peak, query = pl.pallas_call(
        functools.partial(kernel, Z, X, C, D),
        name="decode",
        out_shape=(
            jax.ShapeDtypeStruct(block, BF16),
            jax.ShapeDtypeStruct((8, 128), F32),
            jax.ShapeDtypeStruct(block, BF16),
        ),
        in_specs=[hbm, hbm, hbm, vmem, hbm],
        out_specs=(hbm, vmem, vmem),
        scratch_shapes=[
            pltpu.VMEM((TOK, K), BF16),
            pltpu.VMEM(block, BF16),
            pltpu.VMEM(block, BF16),
            pltpu.VMEM((SLOTS, K, F), BF16),
            pltpu.VMEM((n, F, q_weight.shape[1]), BF16),
            pltpu.VMEM((n,) + block, BF16),
            pltpu.VMEM((Z * X,) + block, F32),
            pltpu.VMEM(block, F32),
            pltpu.VMEM((pairs,) + block, BF16),
            pltpu.VMEM((pairs,) + block, BF16),
            pltpu.VMEM((Z * (X - 1),) + block, BF16),
            pltpu.VMEM((Z * (X - 1),) + block, BF16),
            pltpu.VMEM((Z - 1,) + block, BF16),
            pltpu.VMEM((Z - 1,) + block, BF16),
            pltpu.VMEM((3, 8, 128), F32),
            pltpu.VMEM((hops, 8, 128), F32),
            dma((3,)), dma((SLOTS,)), dma((n,)),
            dma((pairs,)), dma((pairs,)),
            dma((Z * (X - 1),)), dma((Z * (X - 1),)),
            dma((Z - 1,)), dma((Z - 1,)),
            dma((n,)), dma((n,)),
            dma((hops,)), dma((hops,)),
        ],
        compiler_params=pltpu.CompilerParams(
            collective_id=0, has_side_effects=True, vmem_limit_bytes=66 * 1000 * 1000),
    )(attn_heads, residual, o_weight, norm_gain.reshape(1, F), q_weight)
    return hidden, peak[0, :TOK], query


def solution(mesh):
    split = ("tp", "tq", "tr")
    placed = (
        P("groups", split),
        P("groups", split),
        P(split, None),
        P(split),
        P(None, split),
    )
    return jax.shard_map(
        functools.partial(body, tuple(mesh.shape[axis] for axis in split)),
        mesh=mesh,
        in_specs=placed,
        out_specs=(P("groups", split), P("groups"), P("groups", split)),
        check_vma=False,
    )
```

```python
import functools

import jax
import jax.numpy as jnp
from jax import lax
from jax.experimental import pallas as pl
from jax.experimental.pallas import tpu as pltpu
from jax.sharding import PartitionSpec as P

MESH = pl.DeviceIdType.MESH
F32, BF16 = jnp.float32, jnp.bfloat16
SLOTS = 8
PARTS = 2


def flip(index, mask):
    bit = 1
    while bit <= mask:
        if mask & bit:
            index = index + bit - 2 * bit * ((index // bit) % 2)
        bit *= 2
    return index


def multiply(lhs_ref, rhs_ref, put):
    width = rhs_ref.shape[1]
    tile = min(width, 512)

    def step(j, carry):
        columns = pl.ds(pl.multiple_of(j * tile, tile), tile)
        put(columns, jnp.dot(lhs_ref[...], rhs_ref[:, columns], preferred_element_type=F32))
        return carry

    lax.fori_loop(0, width // tile, step, 0)


def kernel(
    Z, X, C, D,
    attn_hbm, res_hbm, o_hbm, gain_ref, q_hbm,
    hidden_hbm, peak_ref, query_ref,
    attn, res, hid, obuf, qbuf, gath, acc, total,
    core_out, core_in, x_out, x_in, z_out, z_in, stat_out, stat_in,
    small_sem, o_sem, q_sem, core_s, core_r, x_s, x_r, z_s, z_r, g_s, g_r, f_s, st_s, st_r,
):
    TOK, F = res.shape
    n = Z * X * C
    me = {"tp": lax.axis_index("tp"), "tq": lax.axis_index("tq"), "tr": lax.axis_index("tr")}

    z = me["tp"]
    line = Z == 4
    inner = jnp.logical_or(z == 1, z == 2)
    outer = jnp.logical_or(z == 0, z == 3)
    rows = [pl.ds(h * (TOK // PARTS), TOK // PARTS) for h in range(PARTS)]
    halves = range(PARTS)

    def z_of(role):
        if line and role == 2:
            return 2 - z // 2
        if line and role == 3:
            return 3 - 3 * (z // 2)
        return flip(z, role)

    def block_of(role, dx, dc):
        return (z_of(role) * X + flip(me["tq"], dx)) * C + flip(me["tr"], dc)

    def remote(src, dst, s, r, axis, d):
        return pltpu.make_async_remote_copy(
            src_ref=src, dst_ref=dst, send_sem=s, recv_sem=r,
            device_id={axis: flip(me[axis], d)}, device_id_type=MESH,
        )

    def send(src, dst, s, r, axis, d, only=None):
        copy = remote(src, dst, s, r, axis, d)
        if only is None:
            copy.start()
        else:
            pl.when(only)(copy.start)
        sent.append((copy, only))
        return copy

    sent = []
    roles = list(reversed(range(Z)))
    groups = [(role, dx) for role in roles for dx in reversed(range(X))]
    order = [(role, dx, dc) for role, dx in groups for dc in reversed(range(C))]

    def o_copy(b):
        start = pl.multiple_of(block_of(*order[b]) * F, F)
        return pltpu.make_async_copy(
            o_hbm.at[:, pl.ds(start, F)], obuf.at[b % SLOTS], o_sem.at[b % SLOTS])

    def slot(role, dx, dc):
        return (role * X + dx) * C + dc

    plan = [("mul", (0, 0, 0))] + [("take", (0, 0, dc)) for dc in range(1, C)]
    plan += [("mul", (0, 0, dc)) for dc in range(1, C)]
    ready = []
    for role in range(1, Z + 1):
        new = [(role, 0, 0)] if role < Z else []
        new += [(role - 1, dx, 0) for dx in range(1, X)]
        for at in new:
            plan.append(("take", at))
            if ready:
                plan.append(("mul", ready.pop(0)))
        ready += new
        while len(ready) > len(new):
            plan.append(("mul", ready.pop(0)))
        later = [(role, 0, dc) for dc in range(1, C)] if role < Z else []
        later += [(role - 1, dx, dc) for dx in range(1, X) for dc in range(1, C)]
        ready += later
    taken = {at for what, at in plan if what == "take"}
    full = []
    for what, at in plan:
        if what == "mul" and at not in taken and at != (0, 0, 0):
            full.append(("take", at))
        full.append((what, at))
    for at in ready:
        if at not in taken:
            full.append(("take", at))
        full.append(("mul", at))
    plan = full
    use = [at for what, at in plan if what == "mul"]

    def q_copy(k):
        start = pl.multiple_of(block_of(*use[k]) * F, F)
        at = slot(*use[k])
        return pltpu.make_async_copy(q_hbm.at[pl.ds(start, F), :], qbuf.at[at], q_sem.at[at])

    attn_copy = pltpu.make_async_copy(attn_hbm, attn, small_sem.at[0])
    attn_copy.start()
    for b in range(min(SLOTS, n)):
        o_copy(b).start()
    res_copy = pltpu.make_async_copy(res_hbm, res, small_sem.at[1])
    res_copy.start()

    barrier = pltpu.get_barrier_semaphore()
    for axis, size in (("tp", Z), ("tq", X), ("tr", C)):
        for d in range(1, size):
            pl.semaphore_signal(
                barrier, inc=1, device_id={axis: flip(me[axis], d)}, device_id_type=MESH)
    attn_copy.wait()
    gain = gain_ref[...].reshape(1, F).astype(F32)

    core_copies, x_copies, z_copies = {}, {}, {}
    q_next = 0

    def after_core(i):
        role, dx = groups[i]
        for h in halves:
            value = acc[i, rows[h]]
            for dc in range(1, C):
                core_copies[i, dc, h].wait_recv()
                value = value + core_in[i * (C - 1) + dc - 1, rows[h]].astype(F32)
            if dx:
                at = role * (X - 1) + dx - 1
                x_out[at, rows[h]] = value.astype(BF16)
                x_copies[role, dx, h] = send(
                    x_out.at[at, rows[h]], x_in.at[at, rows[h]],
                    x_s.at[at, h], x_r.at[at, h], "tq", dx)
            else:
                acc[i, rows[h]] = value

    def z_send(role, to, h, d, only=None):
        z_copies[to, h] = send(
            z_out.at[role - 1, rows[h]], z_in.at[to, rows[h]],
            z_s.at[to, h], z_r.at[to, h], "tp", d, only)

    def after_x(role):
        i = groups.index((role, 0))
        for h in halves:
            value = acc[i, rows[h]]
            for dx in range(1, X):
                x_copies[role, dx, h].wait_recv()
                value = value + x_in[role * (X - 1) + dx - 1, rows[h]].astype(F32)
            if role == 0 or line:
                acc[i, rows[h]] = value
            if role:
                if line:

                    def store(value=value, h=h):
                        z_out[role - 1, rows[h]] = value.astype(BF16)

                    pl.when(outer)(store)
                    z_send(role, 3 - role, h, 1, outer)
                else:
                    z_out[role - 1, rows[h]] = value.astype(BF16)
                    z_send(role, role - 1, h, role)

    def relay(role):
        i = groups.index((role, 0))
        source = {3: 0, 2: 1, 1: 3}[role]
        to, d = {3: (3, 3), 2: (4, 3), 1: (5, 1)}[role]
        for h in halves:

            def add(h=h):
                z_copies[source, h].wait_recv()
                z_out[role - 1, rows[h]] = (
                    acc[i, rows[h]] + z_in[source, rows[h]].astype(F32)).astype(BF16)

            pl.when(inner)(add)
            z_send(role, to, h, d, inner)

    due = {}
    for role in roles[:-1]:
        i = groups.index((role, 0))
        due.setdefault(i + 3, []).append(functools.partial(after_x, role))
        if line:
            due.setdefault(i + 6, []).append(functools.partial(relay, role))
    for i, (role, dx) in enumerate(groups):
        for dc in reversed(range(C)):
            b = i * C + C - 1 - dc
            o_copy(b).wait()
            rhs = obuf.at[b % SLOTS]
            if dc:
                at = i * (C - 1) + dc - 1

                def put(columns, product):
                    core_out[at, :, columns] = product.astype(BF16)

                multiply(attn, rhs, put)
                if b == 0:
                    pl.semaphore_wait(barrier, Z + X + C - 3)
                for h in halves:
                    core_copies[i, dc, h] = send(
                        core_out.at[at, rows[h]], core_in.at[at, rows[h]],
                        core_s.at[at, h], core_r.at[at, h], "tr", dc)
            else:

                def put(columns, product):
                    acc[i, :, columns] = product

                multiply(attn, rhs, put)
            if b + SLOTS < n:
                o_copy(b + SLOTS).start()
            else:
                q_copy(q_next).start()
                q_next += 1
            if dc == C - 1 and i >= 1:
                after_core(i - 1)
        for event in due.pop(i, ()):
            event()
    while q_next < n:
        q_copy(q_next).start()
        q_next += 1
    after_core(len(groups) - 1)
    for when in sorted(due):
        for event in due[when]:
            event()
    after_x(0)

    res_copy.wait()
    last = len(groups) - 1
    if line:
        for h in halves:

            def end(h=h):
                z_copies[5, h].wait_recv()
                total[rows[h]] = acc[last, rows[h]] + z_in[5, rows[h]].astype(F32)

            def middle(h=h):
                z_copies[2, h].wait_recv()
                z_copies[4, h].wait_recv()
                total[rows[h]] = (acc[last, rows[h]] + z_in[2, rows[h]].astype(F32)
                                  + z_in[4, rows[h]].astype(F32))

            pl.when(outer)(end)
            pl.when(inner)(middle)
    else:
        for h in halves:
            value = acc[last, rows[h]]
            for role in range(1, Z):
                z_copies[role - 1, h].wait_recv()
                value = value + z_in[role - 1, rows[h]].astype(F32)
            total[rows[h]] = value

    arrive = {}

    def gather(source, to, h, axis, d, only=None, add=True):
        a, b = slot(*source), slot(*to)
        s = g_s.at[b, h] if add else f_s.at[source[0], h]
        copy = send(gath.at[a, rows[h]], gath.at[b, rows[h]], s, g_r.at[b, h], axis, d, only)
        if add:
            arrive[to, h] = copy

    def spread(at, h):
        role, dx, dc = at
        if dc:
            return
        if dx == 0:
            if line:
                if role == 0:
                    gather(at, (1, 0, 0), h, "tp", 1)
                    gather(at, (2, 0, 0), h, "tp", 3, inner)
                elif role == 1:
                    gather(at, (3, 0, 0), h, "tp", 3, inner)
                else:
                    gather(at, at, h, "tp", 1, inner, add=False)
            elif role == 0:
                for to in range(1, Z):
                    gather(at, (to, 0, 0), h, "tp", to)
            for d in range(1, X):
                gather(at, (role, d, 0), h, "tq", d)
        for d in range(1, C):
            gather(at, (role, dx, d), h, "tr", d)

    for h in halves:
        hidden = (res[rows[h]].astype(F32) + total[rows[h]]).astype(BF16)
        hid[rows[h]] = hidden
        gath[0, rows[h]] = (hidden.astype(F32) * gain).astype(BF16)
        spread((0, 0, 0), h)
    widened = hid[...].astype(F32)
    gained = widened * gain
    hidden_copy = pltpu.make_async_copy(hid, hidden_hbm, small_sem.at[2])
    hidden_copy.start()

    squares = jnp.sum(widened * widened, axis=1, keepdims=True)
    top = jnp.max(jnp.abs(gained), axis=1, keepdims=True)
    wide = jnp.concatenate(
        [jnp.broadcast_to(squares, (TOK, 128)), jnp.broadcast_to(top, (TOK, 128))], axis=0)
    stat = jnp.transpose(wide)[:8, :]
    lane = lax.broadcasted_iota(jnp.int32, stat.shape, 1)
    axes = (("tr", C), ("tq", X), ("tp", Z))
    first = {"tr": 0, "tq": C - 1, "tp": C + X - 2}
    stat_copies = {}

    def stat_send(stage, stat):
        axis, size = axes[stage]
        stat_out[stage] = stat
        for d in range(1, size):
            at = first[axis] + d - 1
            stat_copies[axis, d] = send(
                stat_out.at[stage], stat_in.at[at], st_s.at[at], st_r.at[at], axis, d)

    def stat_take(stage, stat):
        axis, size = axes[stage]
        for d in range(1, size):
            stat_copies[axis, d].wait_recv()
            other = stat_in[first[axis] + d - 1]
            stat = jnp.where(lane < TOK, stat + other, jnp.maximum(stat, other))
        return stat

    stat_send(0, stat)

    k = 0
    for what, at in plan:
        if what == "take":
            for h in halves:
                arrive[at, h].wait_recv()
                spread(at, h)
            continue
        q_copy(k).wait()
        if k == 0:

            def put(columns, product):
                total[:, columns] = product
        else:

            def put(columns, product):
                total[:, columns] += product

        multiply(gath.at[slot(*at)], qbuf.at[slot(*at)], put)
        if k in (1, 3):
            stage = 0 if k == 1 else 1
            stat = stat_take(stage, stat_out[stage])
            stat_send(stage + 1, stat)
        k += 1
    stat = stat_take(2, stat_out[2])
    scale = lax.rsqrt(stat / D + 1e-05)
    peak_ref[...] = pltpu.roll(stat, TOK, 1) * scale
    column = jnp.transpose(jnp.broadcast_to(scale[:1, :], (128, 128)))[:TOK, :1]
    query_ref[...] = (total[...] * column).astype(BF16)
    hidden_copy.wait()
    for copy, only in sent:
        if only is None:
            copy.wait_send()
        else:
            pl.when(only)(copy.wait_send)


def place(hidden_in, peak_in, query_in, hidden_ref, peak_ref, query_ref):
    hidden_ref[...] = hidden_in[...]
    peak_ref[...] = peak_in[0, : peak_ref.shape[0]]
    query_ref[...] = query_in[...]


def body(sizes, attn_heads, residual, o_weight, norm_gain, q_weight):
    Z, X, C = sizes
    TOK, F = residual.shape
    K, D = o_weight.shape
    n = Z * X * C
    pairs = Z * X * (C - 1)
    dma = pltpu.SemaphoreType.DMA
    block = (TOK, F)
    hbm = pl.BlockSpec(memory_space=pl.ANY)
    vmem = pl.BlockSpec(memory_space=pltpu.VMEM)
    hops = C + X + Z - 3
    steps = 6 if Z == 4 else Z - 1
    hidden, peak, query = pl.pallas_call(
        functools.partial(kernel, Z, X, C, D),
        name="decode",
        out_shape=(
            jax.ShapeDtypeStruct(block, BF16),
            jax.ShapeDtypeStruct((8, 128), F32),
            jax.ShapeDtypeStruct(block, BF16),
        ),
        in_specs=[hbm, hbm, hbm, vmem, hbm],
        out_specs=(hbm, vmem, vmem),
        scratch_shapes=[
            pltpu.VMEM((TOK, K), BF16),
            pltpu.VMEM(block, BF16),
            pltpu.VMEM(block, BF16),
            pltpu.VMEM((SLOTS, K, F), BF16),
            pltpu.VMEM((n, F, q_weight.shape[1]), BF16),
            pltpu.VMEM((n,) + block, BF16),
            pltpu.VMEM((Z * X,) + block, F32),
            pltpu.VMEM(block, F32),
            pltpu.VMEM((pairs,) + block, BF16),
            pltpu.VMEM((pairs,) + block, BF16),
            pltpu.VMEM((Z * (X - 1),) + block, BF16),
            pltpu.VMEM((Z * (X - 1),) + block, BF16),
            pltpu.VMEM((Z - 1,) + block, BF16),
            pltpu.VMEM((steps,) + block, BF16),
            pltpu.VMEM((3, 8, 128), F32),
            pltpu.VMEM((hops, 8, 128), F32),
            dma((3,)), dma((SLOTS,)), dma((n,)),
            dma((pairs, PARTS)), dma((pairs, PARTS)),
            dma((Z * (X - 1), PARTS)), dma((Z * (X - 1), PARTS)),
            dma((steps, PARTS)), dma((steps, PARTS)),
            dma((n, PARTS)), dma((n, PARTS)), dma((4, PARTS)),
            dma((hops,)), dma((hops,)),
        ],
        compiler_params=pltpu.CompilerParams(
            collective_id=0, has_side_effects=True, vmem_limit_bytes=66 * 1000 * 1000),
    )(attn_heads, residual, o_weight, norm_gain, q_weight)
    return pl.pallas_call(
        place,
        name="place",
        out_shape=(
            jax.ShapeDtypeStruct(block, BF16),
            jax.ShapeDtypeStruct((TOK,), F32),
            jax.ShapeDtypeStruct(block, BF16),
        ),
        in_specs=[vmem] * 3,
        out_specs=(vmem,) * 3,
    )(hidden, peak, query)


def solution(mesh):
    split = ("tp", "tq", "tr")
    placed = (
        P("groups", split),
        P("groups", split),
        P(split, None),
        P(split),
        P(None, split),
    )
    return jax.shard_map(
        functools.partial(body, tuple(mesh.shape[axis] for axis in split)),
        mesh=mesh,
        in_specs=placed,
        out_specs=(P("groups", split), P("groups"), P("groups", split)),
        check_vma=False,
    )
```
